256 devices in a mesh: dp: 4 (over y), expert: 8 (over z), mp: 8 (over x, core).
Axes of the slice: x: 4, y: 4, z: 8, core: 2. Of those that a mesh axis runs over, the one named last changes fastest.
Arguments:
- base_weights: bfloat16 [16, 2560, 3072], P('expert', None, 'mp'), may hold values from -6 to 6
- delta_blocks: bfloat16 [32768, 128, 128], P(('dp', 'expert', 'mp')), may hold values from -4 to 4
- block_ids: int32 [32768], P(('dp', 'expert', 'mp')), may hold values from 0 to 7679, as said below
- block_counts: int32 [16384], P(('dp', 'expert', 'mp')), may hold values from 0 to 2, as said below
- owner_map: int32 [16], replicated, may hold values from 0 to 15, as said below
Outputs:
- merged_weights: bfloat16 [16, 2560, 3072], P('expert', None, 'mp')
The draws below stay inside these ranges and needn't reach their ends.
Inputs may be any that keep to these rules, and one draw needn't show every extreme that they name: A permutation: expert e is held in serving position owner_map[e], by the serving group owner_map[e] // 2. `block_ids`: every slot of device s for owner q, used or not, names a block (e * 20 + r) * 24 + c with owner_map[e] // 2 == q // 8 and c // 3 == q % 8. Names may repeat within and across devices. `block_counts`: at most 2 used slots from one device to one owner; in every draw some owner receives exactly 2 blocks from every device.
All inputs are finite; a program needn't handle non-finite values.
Results may differ from the reference program's by a relative error of at most 0.001.
Values may be sent and summed in bfloat16 or wider, within the bound.
A program may use at most 128 MiB of HBM per device.

```python
import jax
import jax.numpy as jnp
from jax import lax

BS = 128
DW = 2560
FF2 = 3072
EXP_DEV = 2
CAP = 2
E = 16
N_DEST = 64
RBW = 20
CB = 24
CBD = 3
N_MP = 8
DEVICES = 256


def serving_order(key):
    return jax.random.permutation(jax.random.fold_in(key, 11), E).astype(jnp.int32)


def draw_owner_map(key, part):
    return serving_order(key)


def draw_block_ids(key, part):
    order = serving_order(key)
    inverse = jnp.zeros((E,), jnp.int32).at[order].set(jnp.arange(E, dtype=jnp.int32))
    length = DEVICES * N_DEST * CAP
    slots = jnp.arange(length, dtype=jnp.int32)
    group = slots // CAP % N_DEST
    owner = group // N_MP
    column_part = group % N_MP
    within = jax.random.randint(jax.random.fold_in(key, 31), (length,), 0, EXP_DEV).astype(jnp.int32)
    expert = inverse[owner * EXP_DEV + within]
    row_pick = jax.random.randint(jax.random.fold_in(key, 32), (length,), 0, RBW).astype(jnp.int32)
    col_pick = jax.random.randint(jax.random.fold_in(key, 33), (length,), 0, CBD).astype(jnp.int32)
    column = column_part * CBD + col_pick
    return ((expert * RBW + row_pick) * CB + column).astype(jnp.int32)


def draw_block_counts(key, part):
    tiers = jax.random.randint(jax.random.fold_in(key, 21), (N_DEST,), 0, 4).astype(jnp.int32)
    fullest = jax.random.randint(jax.random.fold_in(key, 22), (), 0, N_DEST).astype(jnp.int32)
    tiers = jnp.where(jnp.arange(N_DEST, dtype=jnp.int32) == fullest, 0, tiers)
    limit = jnp.right_shift(jnp.int32(8), tiers)
    trials = jax.random.randint(jax.random.fold_in(key, 23), (DEVICES, N_DEST, CAP), 0, 8).astype(jnp.int32)
    counts = jnp.sum((trials < limit[None, :, None]).astype(jnp.int32), axis=2)
    return counts.reshape(DEVICES * N_DEST).astype(jnp.int32)


def steps_of(rng, shape, pieces, smallest, high):
    loudness, own = 1.0, jax.random.fold_in(rng, 6)
    for position, parts in pieces:
        heights = jnp.exp(jax.random.uniform(jax.random.fold_in(own, position), (parts,), jnp.float32, smallest / len(pieces), high / len(pieces)))
        loudness = loudness * jnp.repeat(heights, shape[position] // parts).reshape([-1 if axis == position else 1 for axis in range(len(shape))])
    return loudness


def gaussian(own_key, shape, width, bound, pieces=(), kind=jnp.bfloat16):
    entries = jax.random.normal(own_key, shape, jnp.float32) * width
    if len(pieces) > 0:
        entries = steps_of(own_key, shape, pieces, -0.22, 0.18) * entries
    return jnp.clip(entries, min=-bound, max=bound).astype(kind)


def setup_inputs(seed: int = 0) -> dict:
    key_of = jax.random.split(jax.random.key(seed), 6)
    return {
        "base_weights": gaussian(key_of[0], (E, DW, FF2), 1.0, 6.0, ((0, 8), (2, 8))),
        "delta_blocks": gaussian(key_of[1], (DEVICES * N_DEST * CAP, BS, BS), 0.5, 4.0, ((0, 256),)),
        "block_ids": draw_block_ids(jax.random.fold_in(key_of[5], 71), 0),
        "block_counts": draw_block_counts(jax.random.fold_in(key_of[5], 71), 0),
        "owner_map": draw_owner_map(jax.random.fold_in(key_of[5], 71), 0),
    }


def reference(base_weights, delta_blocks, block_ids, block_counts, owner_map):
    slot_count = N_DEST * CAP
    row_blocks = DW // BS
    col_total = FF2 // BS
    block_total = E * row_blocks * col_total
    listed = delta_blocks.reshape(DEVICES, slot_count, BS, BS)
    idents = block_ids.reshape(DEVICES, slot_count)
    counts = block_counts.reshape(DEVICES, N_DEST)
    active = (jnp.arange(slot_count, dtype=jnp.int32) % CAP)[None, :] < jnp.repeat(counts, CAP, axis=1)

    def add_source(running, record):
        values, names, usable = record
        values = jnp.where(usable[:, None, None], values.astype(jnp.float32), jnp.float32(0.0))
        return running.at[names].add(values), None

    start = jnp.zeros((block_total, BS, BS), jnp.float32)
    summed, unused = lax.scan(add_source, start, (listed, idents, active))
    grid = summed.reshape(E, row_blocks, col_total, BS, BS).transpose(0, 1, 3, 2, 4)
    task_delta = grid.reshape(E, DW, FF2)
    serving = jnp.zeros((E, DW, FF2), jnp.float32).at[owner_map].set(task_delta)
    return (base_weights.astype(jnp.float32) + serving).astype(jnp.bfloat16)
```

```python
import functools

import jax
import jax.numpy as jnp
from jax import lax
from jax.experimental import pallas as pl
from jax.experimental.pallas import tpu as pltpu
from jax.sharding import PartitionSpec as P

MESH = pl.DeviceIdType.MESH
ROWS = 8
LANES = 128


def kernel(
    cfg,
    owner_map_ref,
    base_hbm,
    delta_hbm,
    ids_ref,
    counts_ref,
    out_hbm,
    *scratch,
):
    n_dp, n_ex, n_mp, exp_dev, row_blocks, col_blocks, capacity, chunks = cfg
    recv = scratch[:chunks]
    (
    base_vmem,
    partial,
    stage,
    enc,
    keys,
    keys_t,
    table,
    order,
    a2a_send,
    a2a_recv,
    ids_send,
    ids_recv,
    local_sem,
    gather_send,
    gather_recv,
    ) = scratch[chunks:]
    n_dev = n_dp * n_ex * n_mp
    n_slots = n_dev * capacity
    quarter = chunks * ROWS
    positions = exp_dev * row_blocks * col_blocks
    col_total = col_blocks * n_mp
    d = lax.axis_index("dp")
    e = lax.axis_index("expert")
    m = lax.axis_index("mp")
    me = (d * n_ex + e) * n_mp + m

    barrier = pltpu.get_barrier_semaphore()
    ds = [lax.rem(d + i, n_dp) for i in range(n_dp)]
    es = [lax.rem(e + i, n_ex) for i in range(n_ex)]

    def greet(i, carry):
        m2 = lax.rem(m + i, n_mp)
        for j in range(n_dp):
            for k in range(n_ex):
                pl.semaphore_signal(barrier, inc=1, device_id=(ds[j], es[k], m2), device_id_type=MESH)
        return carry

    for j in range(n_dp):
        for k in range(n_ex):
            if j or k:
                pl.semaphore_signal(barrier, inc=1, device_id=(ds[j], es[k], m), device_id_type=MESH)
    lax.fori_loop(1, n_mp, greet, 0)

    base_copy = pltpu.make_async_copy(base_hbm.at[:, :, pl.ds(d * quarter, quarter), :], base_vmem, local_sem.at[0])
    base_copy.start()

    ids = ids_ref[...].astype(jnp.float32)
    per_expert = row_blocks * col_total
    expert = jnp.floor((ids + 0.5) * (1.0 / per_expert))
    remain = ids - expert * per_expert
    row_index = jnp.floor((remain + 0.5) * (1.0 / col_total))
    col_index = remain - row_index * col_total
    part = jnp.floor((col_index + 0.5) * (1.0 / col_blocks))
    local_col = col_index - part * col_blocks
    local_expert = jnp.zeros_like(ids)
    for i in range(n_ex * exp_dev):
        local_expert = jnp.where(expert == i, lax.rem(owner_map_ref[i], exp_dev).astype(jnp.float32), local_expert)
    place = (local_expert * row_blocks + row_index) * col_blocks + local_col
    owners = counts_ref.shape[1]
    spread = (
        lax.broadcasted_iota(jnp.int32, (owners, LANES), 1) // capacity
        == lax.broadcasted_iota(jnp.int32, (owners, LANES), 0)
    ).astype(jnp.float32)
    used = jnp.dot(
        jnp.broadcast_to(counts_ref[...].astype(jnp.float32), (8, owners)), spread, preferred_element_type=jnp.float32
    )[0:1, :]
    slot_k = lax.broadcasted_iota(jnp.int32, (1, LANES), 1) % capacity
    place = jnp.where(slot_k.astype(jnp.float32) < used, place, float(positions))
    enc[...] = place.astype(jnp.int32)

    pl.semaphore_wait(barrier, n_dev - 1)

    z_order = []
    for i in range(1, n_ex // 2):
        z_order += [i, n_ex - i]
    z_order.append(n_ex // 2)

    def send_block(c, d2, e2, m2, with_ids):
        q = e2 * n_mp + m2
        pltpu.make_async_remote_copy(
            src_ref=delta_hbm.at[pl.ds(q * capacity, capacity), pl.ds(d2 * quarter + c * ROWS, ROWS), :],
            dst_ref=recv[c].at[pl.ds(me * capacity, capacity)],
            send_sem=a2a_send.at[c],
            recv_sem=a2a_recv.at[c],
            device_id=(d2, e2, m2),
            device_id_type=MESH,
        ).start()
        if with_ids:
            pltpu.make_async_remote_copy(
                src_ref=enc,
                dst_ref=keys.at[me],
                send_sem=ids_send,
                recv_sem=ids_recv,
                device_id=(d2, e2, m2),
                device_id_type=MESH,
            ).start()

    def exchange(c):
        with_ids = c == 0
        for k in z_order:
            send_block(c, d, es[k], m, with_ids)
        mine = e * n_mp + m
        pltpu.make_async_copy(
            delta_hbm.at[pl.ds(mine * capacity, capacity), pl.ds(d * quarter + c * ROWS, ROWS), :],
            recv[c].at[pl.ds(me * capacity, capacity)],
            a2a_recv.at[c],
        ).start()

        def step(r, carry):
            d2 = lax.rem(d + r // n_mp, n_dp)
            m2 = lax.rem(m + r, n_mp)
            for k in z_order + [0]:
                send_block(c, d2, es[k], m2, with_ids)
            return carry

        lax.fori_loop(1, n_dp * n_mp, step, 0)

    exchange(0)
    keys[pl.ds(me, 1)] = enc[...].reshape(1, 1, LANES)
    if chunks > 1:
        exchange(1)
    base_copy.wait()

    others = keys.at[pl.ds(0, n_dev - 1)]
    pltpu.make_async_copy(others, others, ids_recv).wait()
    all_keys = keys[...].reshape(n_dev, LANES)
    q_mine = e * n_mp + m
    for g in range(n_dev // LANES):
        keys_t[:, g * LANES : (g + 1) * LANES] = all_keys[g * LANES : (g + 1) * LANES, :].T
    lane = lax.broadcasted_iota(jnp.int32, (1, LANES), 1)
    row_keys, row_slots = [], []
    for k in range(capacity):
        row = keys_t[pl.ds(q_mine * capacity + k, 1), :]
        for g in range(n_dev // LANES):
            row_keys.append(row[:, g * LANES : (g + 1) * LANES])
            row_slots.append((g * LANES + lane) * capacity + k)
    groups = len(row_keys)

    def down(row):
        return jnp.broadcast_to(row, (LANES, LANES)).T

    row_mixed = [a * n_slots + b for a, b in zip(row_keys, row_slots)]
    col_keys = [down(a) for a in row_keys]
    col_slots = [down(a) for a in row_slots]
    col_mixed = [a * n_slots + b for a, b in zip(col_keys, col_slots)]

    def count(masks):
        total = sum(jnp.where(x, 1, 0) for x in masks)
        return jnp.sum(total, axis=0, keepdims=True)

    ranks = [count([col_mixed[h] < row_mixed[g] for h in range(groups)]) for g in range(groups)]
    col_ranks = [down(a) for a in ranks]
    for g in range(groups):
        want = g * LANES + lane
        hit = [col_ranks[h] == want for h in range(groups)]
        table[g : g + 1, :] = jnp.sum(sum(jnp.where(x, s, 0) for x, s in zip(hit, col_slots)), axis=0, keepdims=True)
        table[groups + g : groups + g + 1, :] = jnp.sum(
            sum(jnp.where(x, s, 0) for x, s in zip(hit, col_keys)), axis=0, keepdims=True
        )
    table[2 * groups : 2 * groups + 1, :] = jnp.maximum(count([x <= lane for x in col_keys]) - 1, 0)
    table[2 * groups + 1 : 2 * groups + 2, :] = count([x == lane for x in col_keys])

    peers = [lax.rem(d + i, n_dp) for i in range(1, n_dp)]

    for c in range(chunks):
        if c == 0:
            to_smem = pltpu.make_async_copy(table, order, local_sem.at[1])
            to_smem.start()
            to_smem.wait()
        pltpu.make_async_copy(recv[c], recv[c], a2a_recv.at[c]).wait()

        def add(j, carry):
            running, before = carry
            g = j // LANES
            l = j % LANES
            slot = order[g, l]
            key = order[groups + g, l]
            block = recv[c][slot].astype(jnp.float32)
            running = jnp.where(key == before, running, 0.0) + block
            partial[j] = running
            return running, key

        lax.fori_loop(0, n_slots, add, (jnp.zeros((ROWS, LANES), jnp.float32), jnp.int32(-1)), unroll=8)

        def finish(i, carry):
            a = i // row_blocks
            b = i % row_blocks
            for k in range(col_blocks):
                p = i * col_blocks + k
                total = partial[order[2 * groups, p]]
                total = jnp.where(order[2 * groups + 1, p] > 0, total, 0.0)
                old = base_vmem[a, b, c * ROWS : (c + 1) * ROWS, k * LANES : (k + 1) * LANES]
                stage[c, a, b, :, k * LANES : (k + 1) * LANES] = (old.astype(jnp.float32) + total).astype(jnp.bfloat16)
            return carry

        lax.fori_loop(0, exp_dev * row_blocks, finish, 0, unroll=4)
        if c + 2 < chunks:
            exchange(c + 2)
        place_rows = pl.ds(d * quarter + c * ROWS, ROWS)
        for d2 in peers:
            pltpu.make_async_remote_copy(
                src_ref=stage.at[c],
                dst_ref=out_hbm.at[:, :, place_rows, :],
                send_sem=gather_send,
                recv_sem=gather_recv,
                device_id=(d2, e, m),
                device_id_type=MESH,
            ).start()
        pltpu.make_async_copy(stage.at[c], out_hbm.at[:, :, place_rows, :], gather_recv).start()

    pltpu.make_async_copy(out_hbm, out_hbm, gather_recv).wait()
    sent = out_hbm.at[:, :, pl.ds(0, (n_dp - 1) * quarter), :]
    pltpu.make_async_copy(sent, sent, gather_send).wait()
    for c in range(chunks):
        sent = recv[c].at[pl.ds(0, n_slots - capacity)]
        pltpu.make_async_copy(sent, sent, a2a_send.at[c]).wait()
    pltpu.make_async_copy(others, others, ids_send).wait()


def body(base_weights, delta_blocks, block_ids, block_counts, owner_map):
    n_dp, n_ex, n_mp = (lax.axis_size(a) for a in ("dp", "expert", "mp"))
    n_dev = n_dp * n_ex * n_mp
    exp_dev, row_count, col_count = base_weights.shape
    block_size = delta_blocks.shape[1]
    row_blocks = row_count // block_size
    col_blocks = col_count // block_size
    capacity = delta_blocks.shape[0] // block_counts.shape[0]
    quarter = block_size // n_dp
    chunks = quarter // ROWS
    n_slots = n_dev * capacity
    cfg = (n_dp, n_ex, n_mp, exp_dev, row_blocks, col_blocks, capacity, chunks)
    shape = (exp_dev, row_blocks, block_size, col_count)
    merged = pl.pallas_call(
        functools.partial(kernel, cfg),
        out_shape=jax.ShapeDtypeStruct(shape, jnp.bfloat16),
        in_specs=[
            pl.BlockSpec(memory_space=pltpu.SMEM),
            pl.BlockSpec(memory_space=pl.ANY),
            pl.BlockSpec(memory_space=pl.ANY),
            pl.BlockSpec(memory_space=pltpu.VMEM),
            pl.BlockSpec(memory_space=pltpu.VMEM),
        ],
        out_specs=pl.BlockSpec(memory_space=pl.ANY),
        scratch_shapes=[
            *[pltpu.VMEM((n_slots, ROWS, LANES), jnp.bfloat16)] * chunks,
            pltpu.VMEM((exp_dev, row_blocks, quarter, col_count), jnp.bfloat16),
            pltpu.VMEM((n_slots, ROWS, LANES), jnp.float32),
            pltpu.VMEM((chunks, exp_dev, row_blocks, ROWS, col_count), jnp.bfloat16),
            pltpu.VMEM((1, LANES), jnp.int32),
            pltpu.VMEM((n_dev, 1, LANES), jnp.int32),
            pltpu.VMEM((LANES, n_dev), jnp.int32),
            pltpu.VMEM((16, LANES), jnp.int32),
            pltpu.SMEM((16, LANES), jnp.int32),
            pltpu.SemaphoreType.DMA((chunks,)),
            pltpu.SemaphoreType.DMA((chunks,)),
            pltpu.SemaphoreType.DMA,
            pltpu.SemaphoreType.DMA,
            pltpu.SemaphoreType.DMA((2,)),
            pltpu.SemaphoreType.DMA,
            pltpu.SemaphoreType.DMA,
        ],
        compiler_params=pltpu.CompilerParams(
            collective_id=0, has_side_effects=True, vmem_limit_bytes=48 * 2**20
        ),
        name="merge_blocks",
    )(
        owner_map,
        base_weights.reshape(shape),
        delta_blocks,
        block_ids.reshape(1, -1),
        block_counts.reshape(1, -1),
    )
    return merged.reshape(base_weights.shape)


def solution(mesh):
    in_specs = (
        P("expert", None, "mp"),
        P(("dp", "expert", "mp"), None, None),
        P(("dp", "expert", "mp")),
        P(("dp", "expert", "mp")),
        P(),
    )
    out_specs = P("expert", None, "mp")
    return jax.shard_map(body, mesh=mesh, in_specs=in_specs, out_specs=out_specs, check_vma=False)
```

```python
import functools

import jax
import jax.numpy as jnp
from jax import lax
from jax.experimental import pallas as pl
from jax.experimental.pallas import tpu as pltpu
from jax.sharding import PartitionSpec as P

MESH = pl.DeviceIdType.MESH
CHUNKS = (8, 8, 8, 8)
AHEAD = 12
GATHER_SPLITS = 10
PER_STEP = 4
UNROLL = 4
LANES = 128


def kernel(
    cfg,
    lists,
    base_hbm,
    delta_hbm,
    out_hbm,
    *scratch,
):
    n_dp, n_ex, n_mp, exp_dev, row_blocks, col_blocks, capacity, chunk_rows = cfg
    chunks = len(chunk_rows)
    first_row = [sum(chunk_rows[:c]) for c in range(chunks)]
    recv = scratch[:chunks]
    stage = scratch[chunks : 2 * chunks]
    (
        base_vmem,
        partial,
        enc,
        column_keys,
        keys,
        keys_t,
        table,
        flags,
        order,
        weight,
        a2a_send,
        a2a_recv,
        ids_send,
        ids_recv,
        local_sem,
        gather_send,
        gather_recv,
        column_sem,
    ) = scratch[2 * chunks :]
    n_dev = n_dp * n_ex * n_mp
    n_slots = n_dev * capacity
    quarter = sum(chunk_rows)
    positions = exp_dev * row_blocks * col_blocks
    col_total = col_blocks * n_mp
    d = lax.axis_index("dp")
    e = lax.axis_index("expert")
    m = lax.axis_index("mp")
    me = (d * n_mp + m) * n_ex + e

    barrier = pltpu.get_barrier_semaphore()
    ds = [lax.rem(d + i, n_dp) for i in range(n_dp)]
    es = [lax.rem(e + i, n_ex) for i in range(n_ex)]
    ms = [lax.rem(m + i, n_mp) for i in range(n_mp)]
    plane = [(ds[i], e, ms[j]) for j in range(n_mp) for i in range(n_dp) if i or j]
    column = [(d, es[k], m) for k in range(1, n_ex)]
    for device in column + plane:
        pl.semaphore_signal(barrier, inc=1, device_id=device, device_id_type=MESH)

    base_copy = pltpu.make_async_copy(base_hbm.at[:, :, pl.ds(d * quarter, quarter), :], base_vmem, local_sem.at[0])
    base_copy.start()

    ids = lists[0:1, :].astype(jnp.float32)
    counts = lists[1:2, :].astype(jnp.float32)
    owners = n_ex * n_mp
    per_expert = row_blocks * col_total
    expert = jnp.floor((ids + 0.5) * (1.0 / per_expert))
    remain = ids - expert * per_expert
    row_index = jnp.floor((remain + 0.5) * (1.0 / col_total))
    col_index = remain - row_index * col_total
    part = jnp.floor((col_index + 0.5) * (1.0 / col_blocks))
    local_col = col_index - part * col_blocks
    local_expert = jnp.zeros_like(ids)
    for i in range(n_ex * exp_dev):
        position = jnp.broadcast_to(counts[:, owners + i : owners + i + 1], (1, LANES))
        inside = position - exp_dev * jnp.floor(position * (1.0 / exp_dev))
        local_expert = jnp.where(expert == float(i), inside, local_expert)
    place = (local_expert * row_blocks + row_index) * col_blocks + local_col
    spread = (
        lax.broadcasted_iota(jnp.int32, (owners, LANES), 1) // capacity
        == lax.broadcasted_iota(jnp.int32, (owners, LANES), 0)
    ).astype(jnp.float32)
    used = jnp.dot(
        jnp.broadcast_to(counts[:, :owners], (8, owners)), spread, preferred_element_type=jnp.float32
    )[0:1, :]
    slot_k = lax.broadcasted_iota(jnp.int32, (1, LANES), 1) % capacity
    place = jnp.where(slot_k.astype(jnp.float32) < used, place, float(positions))
    enc[...] = place.astype(jnp.int32)

    pl.semaphore_wait(barrier, len(column) + len(plane))
    for device in plane:
        pl.semaphore_signal(column_sem, inc=1, device_id=device, device_id_type=MESH)

    z_order = []
    for i in range(1, n_ex // 2):
        z_order += [i, n_ex - i]
    z_order.append(n_ex // 2)

    def send_block(c, d2, e2, m2):
        q = e2 * n_mp + m2
        pltpu.make_async_remote_copy(
            src_ref=delta_hbm.at[pl.ds(q * capacity, capacity), pl.ds(d2 * quarter + first_row[c], chunk_rows[c]), :],
            dst_ref=recv[c].at[pl.ds(me * capacity, capacity)],
            send_sem=a2a_send.at[c],
            recv_sem=a2a_recv.at[c],
            device_id=(d2, e2, m2),
            device_id_type=MESH,
        ).start()
    mine = e * n_mp + m
    x_count = n_mp // 2
    x = m // 2
    core = m % 2

    n_steps = n_dp * n_mp
    last = chunks - 1
    peers = n_dp - 1
    splits = GATHER_SPLITS
    span = row_blocks // splits
    n_pieces = peers * exp_dev * splits
    half = n_steps // 2
    early = half + AHEAD
    rest_steps = n_steps - early

    def own_pair(c):
        pltpu.make_async_copy(
            delta_hbm.at[pl.ds(mine * capacity, capacity), pl.ds(d * quarter + first_row[c], chunk_rows[c]), :],
            recv[c].at[pl.ds(me * capacity, capacity)],
            a2a_recv.at[c],
        ).start()
        send_block(c, d, e, m + 1 - 2 * core)

    def steps(c, first, stop, gather=None, since=0):
        def step(r, carry):
            side = r // half
            rest = lax.rem(r, half)
            d2 = lax.rem(d + rest // x_count, n_dp)
            m2 = lax.rem(x + rest, x_count) * 2 + side
            for k in z_order:
                send_block(c, d2, es[k], m2)

            @pl.when(rest != 0)
            def _():
                send_block(c, d2, e, m2)

            gather_pieces(gather, r - first + since, PER_STEP)
            return carry

        lax.fori_loop(first, stop, step, 0)

    def gather_pieces(c, step, per_step):
        if c is None:
            return
        for k in range(per_step):
            t = step * per_step + k

            @pl.when(t < n_pieces)
            def _():
                gather_piece(c, t)

    def gather_piece(c, t):
        d2 = lax.rem(d + 1 + t % peers, n_dp)
        a = (t // peers) // splits
        part = pl.ds(((t // peers) % splits) * span, span)
        pltpu.make_async_remote_copy(
            src_ref=stage[c].at[a, part],
            dst_ref=out_hbm.at[a, part, pl.ds(d * quarter + first_row[c], chunk_rows[c]), :],
            send_sem=gather_send,
            recv_sem=gather_recv,
            device_id=(d2, e, m),
            device_id_type=MESH,
        ).start()

    def gather_own(c):
        pltpu.make_async_copy(
            stage[c], out_hbm.at[:, :, pl.ds(d * quarter + first_row[c], chunk_rows[c]), :], gather_recv
        ).start()

    for c in range(chunks):
        own_pair(c)
    for k in range(1, n_ex):
        pltpu.make_async_remote_copy(
            src_ref=enc,
            dst_ref=column_keys.at[e],
            send_sem=ids_send.at[0],
            recv_sem=ids_recv.at[0],
            device_id=(d, es[k], m),
            device_id_type=MESH,
        ).start()
    column_keys[pl.ds(e, 1)] = enc[...].reshape(1, 1, LANES)
    pl.semaphore_wait(column_sem, len(plane))
    steps(0, 0, half)
    others = column_keys.at[pl.ds(0, n_ex - 1)]
    pltpu.make_async_copy(others, others, ids_recv.at[0]).wait()
    here = pl.ds((d * n_mp + m) * n_ex, n_ex)
    for device in plane:
        pltpu.make_async_remote_copy(
            src_ref=column_keys,
            dst_ref=keys.at[here],
            send_sem=ids_send.at[1],
            recv_sem=ids_recv.at[1],
            device_id=device,
            device_id_type=MESH,
        ).start()
    keys[here] = column_keys[...]
    steps(0, half, early + rest_steps * core)
    if chunks > 1:
        steps(1, 0, AHEAD * core)
    base_copy.wait()

    far_keys = keys.at[pl.ds(0, n_dev - n_ex)]
    pltpu.make_async_copy(far_keys, far_keys, ids_recv.at[1]).wait()
    all_keys = keys[...].reshape(n_dev, LANES)
    q_mine = e * n_mp + m
    for g in range(n_dev // LANES):
        keys_t[:, g * LANES : (g + 1) * LANES] = all_keys[g * LANES : (g + 1) * LANES, :].T
    lane = lax.broadcasted_iota(jnp.int32, (1, LANES), 1)
    row_keys, row_slots = [], []
    for k in range(capacity):
        row = keys_t[pl.ds(q_mine * capacity + k, 1), :]
        for g in range(n_dev // LANES):
            row_keys.append(row[:, g * LANES : (g + 1) * LANES])
            row_slots.append((g * LANES + lane) * capacity + k)
    groups = len(row_keys)

    def down(row):
        return jnp.broadcast_to(row, (LANES, LANES)).T

    row_mixed = [a * n_slots + b for a, b in zip(row_keys, row_slots)]
    col_keys = [down(a) for a in row_keys]
    col_slots = [down(a) for a in row_slots]
    col_mixed = [a * n_slots + b for a, b in zip(col_keys, col_slots)]

    def count(masks):
        total = sum(jnp.where(x, 1, 0) for x in masks)
        return jnp.sum(total, axis=0, keepdims=True)

    ranks = [count([col_mixed[h] < row_mixed[g] for h in range(groups)]) for g in range(groups)]
    col_ranks = [down(a) for a in ranks]
    for g in range(groups):
        want = g * LANES + lane

        def at(values, rank):
            return jnp.sum(
                sum(jnp.where(r == rank, v, 0) for r, v in zip(col_ranks, values)), axis=0, keepdims=True
            )

        table[g : g + 1, :] = at(col_slots, want)
        same = jnp.logical_and(at(col_keys, want) == at(col_keys, want - 1), lane > 0)
        flags[g : g + 1, :] = jnp.where(same, 1.0, 0.0)
    begin = count([x < lane for x in col_keys])
    end = count([x <= lane for x in col_keys])
    table[groups : groups + 1, :] = jnp.maximum(end - 1, 0)
    flags[groups : groups + 1, :] = jnp.where(end > begin, 1.0, 0.0)
    for g in range(1, groups):
        cut = jnp.logical_and(begin < g * LANES, end > g * LANES)
        flags[groups + g : groups + g + 1, :] = jnp.where(cut, 1.0, 0.0)

    to_smem = [
        pltpu.make_async_copy(table, order, local_sem.at[1]),
        pltpu.make_async_copy(flags, weight, local_sem.at[5]),
    ]
    for copy in to_smem:
        copy.start()
    for copy in to_smem:
        copy.wait()

    def merge(c):
        rows, top = chunk_rows[c], first_row[c]
        pltpu.make_async_copy(recv[c], recv[c], a2a_recv.at[c]).wait()

        def add(l, running):
            result = []
            for g in range(groups):
                block = recv[c][order[g, l]].astype(jnp.float32)
                total = running[g] * weight[g, l] + block
                partial[g * LANES + l, 0:rows] = total
                result.append(total)
            return tuple(result)

        lax.fori_loop(0, LANES, add, (jnp.zeros((rows, LANES), jnp.float32),) * groups, unroll=UNROLL)
        edges = [partial[g * LANES - 1, 0:rows] for g in range(1, groups)]

        def finish(i, carry):
            a = i // row_blocks
            b = i % row_blocks
            for k in range(col_blocks):
                p = i * col_blocks + k
                total = partial[order[groups, p], 0:rows] * weight[groups, p]
                for g in range(1, groups):
                    total = total + edges[g - 1] * weight[groups + g, p]
                old = base_vmem[a, b, top : top + rows, k * LANES : (k + 1) * LANES]
                stage[c][a, b, :, k * LANES : (k + 1) * LANES] = (old.astype(jnp.float32) + total).astype(jnp.bfloat16)
            return carry

        lax.fori_loop(0, exp_dev * row_blocks, finish, 0, unroll=4)

    for c in range(chunks):
        merge(c)
        gather_own(c)
        steps(c, early + rest_steps * core, n_steps, gather=c)
        done = rest_steps * (1 - core)
        if c + 1 < chunks:
            steps(c + 1, AHEAD * core, early + rest_steps * core, gather=c, since=done)
            done = done + early + (rest_steps - AHEAD) * core
        if c + 2 < chunks:
            steps(c + 2, 0, AHEAD * core, gather=c, since=done)
            done = done + AHEAD * core

        def remaining(t, carry):
            gather_piece(c, t)
            return carry

        if c + 1 == chunks:
            lax.fori_loop(done * PER_STEP, n_pieces, remaining, 0)

    pltpu.make_async_copy(out_hbm, out_hbm, gather_recv).wait()
    sent = out_hbm.at[:, :, pl.ds(0, (n_dp - 1) * quarter), :]
    pltpu.make_async_copy(sent, sent, gather_send).wait()
    for c in range(chunks):
        sent = recv[c].at[pl.ds(0, n_slots - capacity)]
        pltpu.make_async_copy(sent, sent, a2a_send.at[c]).wait()
    pltpu.make_async_copy(others, others, ids_send.at[0]).wait()
    pltpu.make_async_copy(far_keys, far_keys, ids_send.at[1]).wait()


def body(base_weights, delta_blocks, block_ids, block_counts, owner_map):
    n_dp, n_ex, n_mp = (lax.axis_size(a) for a in ("dp", "expert", "mp"))
    n_dev = n_dp * n_ex * n_mp
    exp_dev, row_count, col_count = base_weights.shape
    block_size = delta_blocks.shape[1]
    row_blocks = row_count // block_size
    col_blocks = col_count // block_size
    capacity = delta_blocks.shape[0] // block_counts.shape[0]
    quarter = block_size // n_dp
    chunk_rows = CHUNKS
    n_slots = n_dev * capacity
    cfg = (n_dp, n_ex, n_mp, exp_dev, row_blocks, col_blocks, capacity, chunk_rows)
    shape = (exp_dev, row_blocks, block_size, col_count)
    filler = jnp.zeros((LANES - block_counts.shape[0] - owner_map.shape[0],), jnp.int32)
    lists = jnp.concatenate([block_ids, block_counts, owner_map, filler]).reshape(2, LANES)
    merged = pl.pallas_call(
        functools.partial(kernel, cfg),
        out_shape=jax.ShapeDtypeStruct(shape, jnp.bfloat16),
        in_specs=[
            pl.BlockSpec(memory_space=pltpu.VMEM),
            pl.BlockSpec(memory_space=pl.ANY),
            pl.BlockSpec(memory_space=pl.ANY),
        ],
        out_specs=pl.BlockSpec(memory_space=pl.ANY),
        scratch_shapes=[
            *[pltpu.VMEM((n_slots, rows, LANES), jnp.bfloat16) for rows in chunk_rows],
            *[pltpu.VMEM((exp_dev, row_blocks, rows, col_count), jnp.bfloat16) for rows in chunk_rows],
            pltpu.VMEM((exp_dev, row_blocks, quarter, col_count), jnp.bfloat16),
            pltpu.VMEM((n_slots, max(chunk_rows), LANES), jnp.float32),
            pltpu.VMEM((1, LANES), jnp.int32),
            pltpu.VMEM((n_ex, 1, LANES), jnp.int32),
            pltpu.VMEM((n_dev, 1, LANES), jnp.int32),
            pltpu.VMEM((LANES, n_dev), jnp.int32),
            pltpu.VMEM((8, LANES), jnp.int32),
            pltpu.VMEM((8, LANES), jnp.float32),
            pltpu.SMEM((8, LANES), jnp.int32),
            pltpu.SMEM((8, LANES), jnp.float32),
            pltpu.SemaphoreType.DMA((len(chunk_rows),)),
            pltpu.SemaphoreType.DMA((len(chunk_rows),)),
            pltpu.SemaphoreType.DMA((2,)),
            pltpu.SemaphoreType.DMA((2,)),
            pltpu.SemaphoreType.DMA((6,)),
            pltpu.SemaphoreType.DMA,
            pltpu.SemaphoreType.DMA,
            pltpu.SemaphoreType.REGULAR,
        ],
        compiler_params=pltpu.CompilerParams(
            collective_id=0, has_side_effects=True, vmem_limit_bytes=48 * 2**20
        ),
        name="merge_blocks",
    )(
        lists,
        base_weights.reshape(shape),
        delta_blocks,
    )
    return merged.reshape(base_weights.shape)


def solution(mesh):
    in_specs = (
        P("expert", None, "mp"),
        P(("dp", "expert", "mp"), None, None),
        P(("dp", "expert", "mp")),
        P(("dp", "expert", "mp")),
        P(),
    )
    out_specs = P("expert", None, "mp")
    return jax.shard_map(body, mesh=mesh, in_specs=in_specs, out_specs=out_specs, check_vma=False)
```

```python
import functools

import jax
import jax.numpy as jnp
from jax import lax
from jax.experimental import pallas as pl
from jax.experimental.pallas import tpu as pltpu
from jax.sharding import PartitionSpec as P

MESH = pl.DeviceIdType.MESH
CHUNKS = (8, 8, 8, 8)
AHEAD = 14
GATHER_SPLITS = 10
PER_STEP = 4
LAST_STEP = 30
FIN_UNROLL = 8
UNROLL = 8
LANES = 128


def kernel(
    cfg,
    lists,
    base_hbm,
    delta_hbm,
    out_hbm,
    *scratch,
):
    n_dp, n_ex, n_mp, exp_dev, row_blocks, col_blocks, capacity, chunk_rows = cfg
    chunks = len(chunk_rows)
    first_row = [sum(chunk_rows[:c]) for c in range(chunks)]
    recv = scratch[:chunks]
    stage = scratch[chunks : 2 * chunks]
    (
        base_vmem,
        partial,
        enc,
        column_keys,
        keys,
        keys_t,
        table,
        flags,
        order,
        weight,
        a2a_send,
        a2a_recv,
        ids_send,
        ids_recv,
        local_sem,
        gather_send,
        gather_recv,
        column_sem,
    ) = scratch[2 * chunks :]
    n_dev = n_dp * n_ex * n_mp
    n_slots = n_dev * capacity
    quarter = sum(chunk_rows)
    positions = exp_dev * row_blocks * col_blocks
    col_total = col_blocks * n_mp
    d = lax.axis_index("dp")
    e = lax.axis_index("expert")
    m = lax.axis_index("mp")
    me = (d * n_mp + m) * n_ex + e

    barrier = pltpu.get_barrier_semaphore()
    ds = [lax.rem(d + i, n_dp) for i in range(n_dp)]
    es = [lax.rem(e + i, n_ex) for i in range(n_ex)]
    ms = [lax.rem(m + i, n_mp) for i in range(n_mp)]
    plane = [(ds[i], e, ms[j]) for j in range(n_mp) for i in range(n_dp) if i or j]
    column = [(d, es[k], m) for k in range(1, n_ex)]
    for device in column + plane:
        pl.semaphore_signal(barrier, inc=1, device_id=device, device_id_type=MESH)

    base_copy = pltpu.make_async_copy(base_hbm.at[:, :, pl.ds(d * quarter, quarter), :], base_vmem, local_sem.at[0])
    base_copy.start()

    ids = lists[0:1, :].astype(jnp.float32)
    counts = lists[1:2, :].astype(jnp.float32)
    owners = n_ex * n_mp
    per_expert = row_blocks * col_total
    expert = jnp.floor((ids + 0.5) * (1.0 / per_expert))
    remain = ids - expert * per_expert
    row_index = jnp.floor((remain + 0.5) * (1.0 / col_total))
    col_index = remain - row_index * col_total
    part = jnp.floor((col_index + 0.5) * (1.0 / col_blocks))
    local_col = col_index - part * col_blocks
    local_expert = jnp.zeros_like(ids)
    for i in range(n_ex * exp_dev):
        position = jnp.broadcast_to(counts[:, owners + i : owners + i + 1], (1, LANES))
        inside = position - exp_dev * jnp.floor(position * (1.0 / exp_dev))
        local_expert = jnp.where(expert == float(i), inside, local_expert)
    place = (local_expert * row_blocks + row_index) * col_blocks + local_col
    spread = (
        lax.broadcasted_iota(jnp.int32, (owners, LANES), 1) // capacity
        == lax.broadcasted_iota(jnp.int32, (owners, LANES), 0)
    ).astype(jnp.float32)
    used = jnp.dot(
        jnp.broadcast_to(counts[:, :owners], (8, owners)), spread, preferred_element_type=jnp.float32
    )[0:1, :]
    slot_k = lax.broadcasted_iota(jnp.int32, (1, LANES), 1) % capacity
    place = jnp.where(slot_k.astype(jnp.float32) < used, place, float(positions))
    enc[...] = place.astype(jnp.int32)

    pl.semaphore_wait(barrier, len(column) + len(plane))
    for device in plane:
        pl.semaphore_signal(column_sem, inc=1, device_id=device, device_id_type=MESH)

    z_order = []
    for i in range(1, n_ex // 2):
        z_order += [i, n_ex - i]
    z_order.append(n_ex // 2)

    def send_block(c, d2, e2, m2):
        q = e2 * n_mp + m2
        pltpu.make_async_remote_copy(
            src_ref=delta_hbm.at[pl.ds(q * capacity, capacity), pl.ds(d2 * quarter + first_row[c], chunk_rows[c]), :],
            dst_ref=recv[c].at[pl.ds(me * capacity, capacity)],
            send_sem=a2a_send.at[c],
            recv_sem=a2a_recv.at[c],
            device_id=(d2, e2, m2),
            device_id_type=MESH,
        ).start()
    mine = e * n_mp + m
    x_count = n_mp // 2
    x = m // 2
    core = m % 2
    late = 1 - core

    n_steps = n_dp * n_mp
    last = chunks - 1
    peers = n_dp - 1
    shifts = [n_dp // 2] + [i for i in range(1, n_dp) if i != n_dp // 2]
    splits = GATHER_SPLITS
    span = row_blocks // splits
    n_pieces = peers * exp_dev * splits
    half = n_steps // 2
    early = half + AHEAD
    rest_steps = n_steps - early

    def known(c):
        pltpu.make_async_copy(
            delta_hbm.at[pl.ds(mine * capacity, capacity), pl.ds(d * quarter + first_row[c], chunk_rows[c]), :],
            recv[c].at[pl.ds(me * capacity, capacity)],
            a2a_recv.at[c],
        ).start()
        for k in z_order:
            send_block(c, d, es[k], m)
        send_block(c, d, e, m + 1 - 2 * core)

    def steps(c, first, stop, gather=None, since=0):
        def step(r, carry):
            side = 1 - r // half
            rest = lax.rem(r, half)
            d2 = lax.rem(d + rest // x_count, n_dp)
            m2 = lax.rem(x + rest, x_count) * 2 + side

            @pl.when(r != half * late)
            def _():
                for k in z_order:
                    send_block(c, d2, es[k], m2)

            @pl.when(rest != 0)
            def _():
                send_block(c, d2, e, m2)

            gather_pieces(gather, r - first + since, PER_STEP if gather != last else LAST_STEP)
            return carry

        lax.fori_loop(first, stop, step, 0)

    def gather_pieces(c, step, per_step):
        if c is None:
            return
        for k in range(per_step):
            t = step * per_step + k

            @pl.when(t < n_pieces)
            def _():
                gather_piece(c, t)

    def gather_piece(c, t):
        d2 = lax.rem(d + 1 + t % peers, n_dp)
        a = (t // peers) // splits
        part = pl.ds(((t // peers) % splits) * span, span)
        pltpu.make_async_remote_copy(
            src_ref=stage[c].at[a, part],
            dst_ref=out_hbm.at[a, part, pl.ds(d * quarter + first_row[c], chunk_rows[c]), :],
            send_sem=gather_send,
            recv_sem=gather_recv,
            device_id=(d2, e, m),
            device_id_type=MESH,
        ).start()

    def gather_row(c, i):
        a = i // row_blocks
        b = lax.rem(i, row_blocks)
        for shift in shifts:
            pltpu.make_async_remote_copy(
                src_ref=stage[c].at[a, b],
                dst_ref=out_hbm.at[a, b, pl.ds(d * quarter + first_row[c], chunk_rows[c]), :],
                send_sem=gather_send,
                recv_sem=gather_recv,
                device_id=(ds[shift], e, m),
                device_id_type=MESH,
            ).start()

    def gather_own(c):
        pltpu.make_async_copy(
            stage[c], out_hbm.at[:, :, pl.ds(d * quarter + first_row[c], chunk_rows[c]), :], gather_recv
        ).start()

    for c in range(chunks):
        known(c)
    for k in range(1, n_ex):
        pltpu.make_async_remote_copy(
            src_ref=enc,
            dst_ref=column_keys.at[e],
            send_sem=ids_send.at[0],
            recv_sem=ids_recv.at[0],
            device_id=(d, es[k], m),
            device_id_type=MESH,
        ).start()
    column_keys[pl.ds(e, 1)] = enc[...].reshape(1, 1, LANES)
    pl.semaphore_wait(column_sem, len(plane))
    steps(0, 0, half)
    others = column_keys.at[pl.ds(0, n_ex - 1)]
    pltpu.make_async_copy(others, others, ids_recv.at[0]).wait()
    here = pl.ds((d * n_mp + m) * n_ex, n_ex)
    for device in plane:
        pltpu.make_async_remote_copy(
            src_ref=column_keys,
            dst_ref=keys.at[here],
            send_sem=ids_send.at[1],
            recv_sem=ids_recv.at[1],
            device_id=device,
            device_id_type=MESH,
        ).start()
    keys[here] = column_keys[...]
    steps(0, half, early + rest_steps * late)
    if chunks > 1:
        steps(1, 0, AHEAD * late)
    base_copy.wait()

    far_keys = keys.at[pl.ds(0, n_dev - n_ex)]
    pltpu.make_async_copy(far_keys, far_keys, ids_recv.at[1]).wait()
    all_keys = keys[...].reshape(n_dev, LANES)
    q_mine = e * n_mp + m
    for g in range(n_dev // LANES):
        keys_t[:, g * LANES : (g + 1) * LANES] = all_keys[g * LANES : (g + 1) * LANES, :].T
    lane = lax.broadcasted_iota(jnp.int32, (1, LANES), 1)
    row_keys, row_slots = [], []
    for k in range(capacity):
        row = keys_t[pl.ds(q_mine * capacity + k, 1), :]
        for g in range(n_dev // LANES):
            row_keys.append(row[:, g * LANES : (g + 1) * LANES])
            row_slots.append((g * LANES + lane) * capacity + k)
    groups = len(row_keys)

    def down(row):
        return jnp.broadcast_to(row, (LANES, LANES)).T

    row_mixed = [a * n_slots + b for a, b in zip(row_keys, row_slots)]
    col_keys = [down(a) for a in row_keys]
    col_slots = [down(a) for a in row_slots]
    col_mixed = [a * n_slots + b for a, b in zip(col_keys, col_slots)]

    def count(masks):
        total = sum(jnp.where(x, 1, 0) for x in masks)
        return jnp.sum(total, axis=0, keepdims=True)

    ranks = [count([col_mixed[h] < row_mixed[g] for h in range(groups)]) for g in range(groups)]
    col_ranks = [down(a) for a in ranks]
    for g in range(groups):
        want = g * LANES + lane

        def at(values, rank):
            return jnp.sum(
                sum(jnp.where(r == rank, v, 0) for r, v in zip(col_ranks, values)), axis=0, keepdims=True
            )

        table[g : g + 1, :] = at(col_slots, want)
        same = jnp.logical_and(at(col_keys, want) == at(col_keys, want - 1), lane > 0)
        flags[g : g + 1, :] = jnp.where(same, 1.0, 0.0)
    begin = count([x < lane for x in col_keys])
    end = count([x <= lane for x in col_keys])
    table[groups : groups + 1, :] = jnp.maximum(end - 1, 0)
    flags[groups : groups + 1, :] = jnp.where(end > begin, 1.0, 0.0)
    for g in range(1, groups):
        cut = jnp.logical_and(begin < g * LANES, end > g * LANES)
        flags[groups + g : groups + g + 1, :] = jnp.where(cut, 1.0, 0.0)

    to_smem = [
        pltpu.make_async_copy(table, order, local_sem.at[1]),
        pltpu.make_async_copy(flags, weight, local_sem.at[5]),
    ]
    for copy in to_smem:
        copy.start()
    for copy in to_smem:
        copy.wait()

    def merge(c):
        rows, top = chunk_rows[c], first_row[c]
        pltpu.make_async_copy(recv[c], recv[c], a2a_recv.at[c]).wait()

        def add(l, running):
            result = []
            for g in range(groups):
                block = recv[c][order[g, l]].astype(jnp.float32)
                total = running[g] * weight[g, l] + block
                partial[g * LANES + l, 0:rows] = total
                result.append(total)
            return tuple(result)

        lax.fori_loop(0, LANES, add, (jnp.zeros((rows, LANES), jnp.float32),) * groups, unroll=UNROLL)
        edges = [partial[g * LANES - 1, 0:rows] for g in range(1, groups)]

        def finish(i, carry):
            a = i // row_blocks
            b = i % row_blocks
            for k in range(col_blocks):
                p = i * col_blocks + k
                total = partial[order[groups, p], 0:rows] * weight[groups, p]
                for g in range(1, groups):
                    total = total + edges[g - 1] * weight[groups + g, p]
                old = base_vmem[a, b, top : top + rows, k * LANES : (k + 1) * LANES]
                stage[c][a, b, :, k * LANES : (k + 1) * LANES] = (old.astype(jnp.float32) + total).astype(jnp.bfloat16)
            if c == last:

                @pl.when(jnp.logical_and(late == 1, i > 0))
                def _():
                    gather_row(c, i - 1)

            return carry

        lax.fori_loop(0, exp_dev * row_blocks, finish, 0, unroll=FIN_UNROLL)
        if c == last:

            @pl.when(late == 1)
            def _():
                gather_row(c, exp_dev * row_blocks - 1)


    for c in range(chunks):
        merge(c)
        gather_own(c)
        if c == last:
            steps(c, early + rest_steps * late, n_steps, gather=c)

            def remaining(t, carry):
                gather_piece(c, t)
                return carry

            lax.fori_loop(rest_steps * LAST_STEP + (n_pieces - rest_steps * LAST_STEP) * late, n_pieces, remaining, 0)
            continue
        steps(c, early + rest_steps * late, n_steps, gather=c)
        done = rest_steps * core
        steps(c + 1, AHEAD * late, early + rest_steps * late, gather=c, since=done)
        if c + 2 < chunks:
            done = done + early + (rest_steps - AHEAD) * late
            steps(c + 2, 0, AHEAD * late, gather=c, since=done)

    pltpu.make_async_copy(out_hbm, out_hbm, gather_recv).wait()
    sent = out_hbm.at[:, :, pl.ds(0, (n_dp - 1) * quarter), :]
    pltpu.make_async_copy(sent, sent, gather_send).wait()
    for c in range(chunks):
        sent = recv[c].at[pl.ds(0, n_slots - capacity)]
        pltpu.make_async_copy(sent, sent, a2a_send.at[c]).wait()
    pltpu.make_async_copy(others, others, ids_send.at[0]).wait()
    pltpu.make_async_copy(far_keys, far_keys, ids_send.at[1]).wait()


def body(base_weights, delta_blocks, block_ids, block_counts, owner_map):
    n_dp, n_ex, n_mp = (lax.axis_size(a) for a in ("dp", "expert", "mp"))
    n_dev = n_dp * n_ex * n_mp
    exp_dev, row_count, col_count = base_weights.shape
    block_size = delta_blocks.shape[1]
    row_blocks = row_count // block_size
    col_blocks = col_count // block_size
    capacity = delta_blocks.shape[0] // block_counts.shape[0]
    quarter = block_size // n_dp
    chunk_rows = CHUNKS
    n_slots = n_dev * capacity
    cfg = (n_dp, n_ex, n_mp, exp_dev, row_blocks, col_blocks, capacity, chunk_rows)
    shape = (exp_dev, row_blocks, block_size, col_count)
    filler = jnp.zeros((LANES - block_counts.shape[0] - owner_map.shape[0],), jnp.int32)
    lists = jnp.concatenate([block_ids, block_counts, owner_map, filler]).reshape(2, LANES)
    merged = pl.pallas_call(
        functools.partial(kernel, cfg),
        out_shape=jax.ShapeDtypeStruct(shape, jnp.bfloat16),
        in_specs=[
            pl.BlockSpec(memory_space=pltpu.VMEM),
            pl.BlockSpec(memory_space=pl.ANY),
            pl.BlockSpec(memory_space=pl.ANY),
        ],
        out_specs=pl.BlockSpec(memory_space=pl.ANY),
        scratch_shapes=[
            *[pltpu.VMEM((n_slots, rows, LANES), jnp.bfloat16) for rows in chunk_rows],
            *[pltpu.VMEM((exp_dev, row_blocks, rows, col_count), jnp.bfloat16) for rows in chunk_rows],
            pltpu.VMEM((exp_dev, row_blocks, quarter, col_count), jnp.bfloat16),
            pltpu.VMEM((n_slots, max(chunk_rows), LANES), jnp.float32),
            pltpu.VMEM((1, LANES), jnp.int32),
            pltpu.VMEM((n_ex, 1, LANES), jnp.int32),
            pltpu.VMEM((n_dev, 1, LANES), jnp.int32),
            pltpu.VMEM((LANES, n_dev), jnp.int32),
            pltpu.VMEM((8, LANES), jnp.int32),
            pltpu.VMEM((8, LANES), jnp.float32),
            pltpu.SMEM((8, LANES), jnp.int32),
            pltpu.SMEM((8, LANES), jnp.float32),
            pltpu.SemaphoreType.DMA((len(chunk_rows),)),
            pltpu.SemaphoreType.DMA((len(chunk_rows),)),
            pltpu.SemaphoreType.DMA((2,)),
            pltpu.SemaphoreType.DMA((2,)),
            pltpu.SemaphoreType.DMA((6,)),
            pltpu.SemaphoreType.DMA,
            pltpu.SemaphoreType.DMA,
            pltpu.SemaphoreType.REGULAR,
        ],
        compiler_params=pltpu.CompilerParams(
            collective_id=0, has_side_effects=True, vmem_limit_bytes=48 * 2**20
        ),
        name="merge_blocks",
    )(
        lists,
        base_weights.reshape(shape),
        delta_blocks,
    )
    return merged.reshape(base_weights.shape)


def solution(mesh):
    in_specs = (
        P("expert", None, "mp"),
        P(("dp", "expert", "mp"), None, None),
        P(("dp", "expert", "mp")),
        P(("dp", "expert", "mp")),
        P(),
    )
    out_specs = P("expert", None, "mp")
    return jax.shard_map(body, mesh=mesh, in_specs=in_specs, out_specs=out_specs, check_vma=False)
```

```python
import functools

import jax
import jax.numpy as jnp
from jax import lax
from jax.experimental import pallas as pl
from jax.experimental.pallas import tpu as pltpu
from jax.sharding import PartitionSpec as P

MESH = pl.DeviceIdType.MESH
CHUNKS = (8, 8, 8, 8)
AHEAD = 16
GATHER_SPLITS = 10
PER_STEP = 4
LAST_STEP = 10
FIN_UNROLL = 8
SEGMENTS = 4
SEGMENT_PARTS = 2
SEG_UNROLL = 10
AHEAD_LAST = 10
UNROLL = 8
LANES = 128


def kernel(
    cfg,
    lists,
    base_hbm,
    delta_hbm,
    out_hbm,
    *scratch,
):
    n_dp, n_ex, n_mp, exp_dev, row_blocks, col_blocks, capacity, chunk_rows = cfg
    chunks = len(chunk_rows)
    first_row = [sum(chunk_rows[:c]) for c in range(chunks)]
    recv = scratch[:chunks]
    stage = scratch[chunks : 2 * chunks]
    (
        base_vmem,
        partial,
        enc,
        column_keys,
        keys,
        keys_t,
        table,
        flags,
        order,
        weight,
        a2a_send,
        a2a_recv,
        ids_send,
        ids_recv,
        local_sem,
        gather_send,
        gather_recv,
        near_recv,
        column_sem,
    ) = scratch[2 * chunks :]
    n_dev = n_dp * n_ex * n_mp
    n_slots = n_dev * capacity
    quarter = sum(chunk_rows)
    positions = exp_dev * row_blocks * col_blocks
    col_total = col_blocks * n_mp
    d = lax.axis_index("dp")
    e = lax.axis_index("expert")
    m = lax.axis_index("mp")
    me = (d * n_mp + m) * n_ex + e

    barrier = pltpu.get_barrier_semaphore()
    ds = [lax.rem(d + i, n_dp) for i in range(n_dp)]
    es = [lax.rem(e + i, n_ex) for i in range(n_ex)]
    ms = [lax.rem(m + i, n_mp) for i in range(n_mp)]
    plane = [(ds[i], e, ms[j]) for j in range(n_mp) for i in range(n_dp) if i or j]
    column = [(d, es[k], m) for k in range(1, n_ex)]
    for device in column + plane:
        pl.semaphore_signal(barrier, inc=1, device_id=device, device_id_type=MESH)

    base_copy = pltpu.make_async_copy(base_hbm.at[:, :, pl.ds(d * quarter, quarter), :], base_vmem, local_sem.at[0])
    base_copy.start()

    ids = lists[0:1, :].astype(jnp.float32)
    counts = lists[1:2, :].astype(jnp.float32)
    owners = n_ex * n_mp
    per_expert = row_blocks * col_total
    expert = jnp.floor((ids + 0.5) * (1.0 / per_expert))
    remain = ids - expert * per_expert
    row_index = jnp.floor((remain + 0.5) * (1.0 / col_total))
    col_index = remain - row_index * col_total
    part = jnp.floor((col_index + 0.5) * (1.0 / col_blocks))
    local_col = col_index - part * col_blocks
    local_expert = jnp.zeros_like(ids)
    for i in range(n_ex * exp_dev):
        position = jnp.broadcast_to(counts[:, owners + i : owners + i + 1], (1, LANES))
        inside = position - exp_dev * jnp.floor(position * (1.0 / exp_dev))
        local_expert = jnp.where(expert == float(i), inside, local_expert)
    place = (local_expert * row_blocks + row_index) * col_blocks + local_col
    spread = (
        lax.broadcasted_iota(jnp.int32, (owners, LANES), 1) // capacity
        == lax.broadcasted_iota(jnp.int32, (owners, LANES), 0)
    ).astype(jnp.float32)
    used = jnp.dot(
        jnp.broadcast_to(counts[:, :owners], (8, owners)), spread, preferred_element_type=jnp.float32
    )[0:1, :]
    slot_k = lax.broadcasted_iota(jnp.int32, (1, LANES), 1) % capacity
    place = jnp.where(slot_k.astype(jnp.float32) < used, place, float(positions))
    enc[...] = place.astype(jnp.int32)

    pl.semaphore_wait(barrier, len(column) + len(plane))
    for device in plane:
        pl.semaphore_signal(column_sem, inc=1, device_id=device, device_id_type=MESH)

    z_order = [n_ex // 2]
    for i in range(n_ex // 2 - 1, 0, -1):
        z_order += [i, n_ex - i]

    def send_block(c, d2, e2, m2):
        q = e2 * n_mp + m2
        pltpu.make_async_remote_copy(
            src_ref=delta_hbm.at[pl.ds(q * capacity, capacity), pl.ds(d2 * quarter + first_row[c], chunk_rows[c]), :],
            dst_ref=recv[c].at[pl.ds(me * capacity, capacity)],
            send_sem=a2a_send.at[c],
            recv_sem=a2a_recv.at[c],
            device_id=(d2, e2, m2),
            device_id_type=MESH,
        ).start()
    mine = e * n_mp + m
    x_count = n_mp // 2
    x = m // 2
    core = m % 2
    late = 1 - core

    n_steps = n_dp * n_mp
    last = chunks - 1
    peers = n_dp - 1
    splits = GATHER_SPLITS
    span = row_blocks // splits
    n_pieces = peers * exp_dev * splits
    half = n_steps // 2
    early = half + AHEAD
    rest_steps = n_steps - early

    def known(c):
        pltpu.make_async_copy(
            delta_hbm.at[pl.ds(mine * capacity, capacity), pl.ds(d * quarter + first_row[c], chunk_rows[c]), :],
            recv[c].at[pl.ds(me * capacity, capacity)],
            a2a_recv.at[c],
        ).start()
        for k in z_order:
            send_block(c, d, es[k], m)
        send_block(c, d, e, m + 1 - 2 * core)

    def steps(c, first, stop, gather=None, since=0):
        def step(r, carry):
            side = 1 - r // half
            rest = lax.rem(r, half)
            d2 = lax.rem(d + rest // x_count, n_dp)
            m2 = lax.rem(x + rest, x_count) * 2 + side

            @pl.when(r != half * late)
            def _():
                for k in z_order:
                    send_block(c, d2, es[k], m2)

            if c == 0:

                @pl.when(rest != 0)
                def _():
                    for other in range(chunks):
                        send_block(other, d2, e, m2)

            gather_pieces(gather, r - first + since, PER_STEP if gather != last else LAST_STEP)
            return carry

        lax.fori_loop(first, stop, step, 0)

    def gather_pieces(c, step, per_step):
        if c is None:
            return
        for k in range(per_step):
            t = step * per_step + k

            @pl.when(t < pieces_of[c])
            def _():
                gather_piece(c, t)

    def rows_of(device, c):
        return pl.ds(device * quarter + first_row[c], chunk_rows[c])

    left, right = ds[n_dp - 1], ds[1]
    pieces_of = [exp_dev * splits * (peers if c == last else 2) for c in range(chunks)]

    def gather_piece(c, t):
        fan = peers if c == last else 2
        piece = t // fan
        a = piece // splits
        part = pl.ds((piece % splits) * span, span)
        to = lax.rem(d + 1 + t % fan * (1 if c == last else n_dp - 2), n_dp)
        arrival = gather_recv if c == last else near_recv.at[c * 2 + t % fan]
        pltpu.make_async_remote_copy(
            src_ref=stage[c].at[a, part],
            dst_ref=out_hbm.at[a, part, rows_of(d, c), :],
            send_sem=gather_send,
            recv_sem=arrival,
            device_id=(to, e, m),
            device_id_type=MESH,
        ).start()

    def forward(c):
        for side in range(2):
            pltpu.make_async_copy(stage[c], stage[c], near_recv.at[c * 2 + side]).wait()

        def step(t, carry):
            part = pl.ds(t * span, span)
            for a in range(exp_dev):
                source, to = (left, right) if a < exp_dev // 2 else (right, left)
                block = out_hbm.at[a, part, rows_of(source, c), :]
                pltpu.make_async_remote_copy(
                    src_ref=block,
                    dst_ref=block,
                    send_sem=gather_send,
                    recv_sem=gather_recv,
                    device_id=(to, e, m),
                    device_id_type=MESH,
                ).start()
            return carry

        lax.fori_loop(0, splits, step, 0)

    def gather_own(c):
        pltpu.make_async_copy(
            stage[c], out_hbm.at[:, :, pl.ds(d * quarter + first_row[c], chunk_rows[c]), :], gather_recv
        ).start()

    for c in range(chunks):
        known(c)
    for k in range(1, n_ex):
        pltpu.make_async_remote_copy(
            src_ref=enc,
            dst_ref=column_keys.at[e],
            send_sem=ids_send.at[0],
            recv_sem=ids_recv.at[0],
            device_id=(d, es[k], m),
            device_id_type=MESH,
        ).start()
    column_keys[pl.ds(e, 1)] = enc[...].reshape(1, 1, LANES)
    pl.semaphore_wait(column_sem, len(plane))
    steps(0, 0, half)
    others = column_keys.at[pl.ds(0, n_ex - 1)]
    pltpu.make_async_copy(others, others, ids_recv.at[0]).wait()
    here = pl.ds((d * n_mp + m) * n_ex, n_ex)
    for device in plane:
        pltpu.make_async_remote_copy(
            src_ref=column_keys,
            dst_ref=keys.at[here],
            send_sem=ids_send.at[1],
            recv_sem=ids_recv.at[1],
            device_id=device,
            device_id_type=MESH,
        ).start()
    keys[here] = column_keys[...]
    steps(0, half, early + rest_steps * late)
    if chunks > 1:
        steps(1, 0, AHEAD * late)
    base_copy.wait()

    far_keys = keys.at[pl.ds(0, n_dev - n_ex)]
    pltpu.make_async_copy(far_keys, far_keys, ids_recv.at[1]).wait()
    all_keys = keys[...].reshape(n_dev, LANES)
    q_mine = e * n_mp + m
    for g in range(n_dev // LANES):
        keys_t[:, g * LANES : (g + 1) * LANES] = all_keys[g * LANES : (g + 1) * LANES, :].T
    lane = lax.broadcasted_iota(jnp.int32, (1, LANES), 1)
    row_keys, row_slots = [], []
    for k in range(capacity):
        row = keys_t[pl.ds(q_mine * capacity + k, 1), :]
        for g in range(n_dev // LANES):
            row_keys.append(row[:, g * LANES : (g + 1) * LANES])
            row_slots.append((g * LANES + lane) * capacity + k)
    groups = len(row_keys)

    def down(row):
        return jnp.broadcast_to(row, (LANES, LANES)).T

    row_mixed = [a * n_slots + b for a, b in zip(row_keys, row_slots)]
    col_keys = [down(a) for a in row_keys]
    col_slots = [down(a) for a in row_slots]
    col_mixed = [a * n_slots + b for a, b in zip(col_keys, col_slots)]

    def count(masks):
        total = sum(jnp.where(x, 1, 0) for x in masks)
        return jnp.sum(total, axis=0, keepdims=True)

    ranks = [count([col_mixed[h] < row_mixed[g] for h in range(groups)]) for g in range(groups)]
    col_ranks = [down(a) for a in ranks]
    for g in range(groups):
        want = g * LANES + lane

        def at(values, rank):
            return jnp.sum(
                sum(jnp.where(r == rank, v, 0) for r, v in zip(col_ranks, values)), axis=0, keepdims=True
            )

        table[g : g + 1, :] = at(col_slots, want)
        same = jnp.logical_and(at(col_keys, want) == at(col_keys, want - 1), lane > 0)
        flags[g : g + 1, :] = jnp.where(same, 1.0, 0.0)
    begin = count([x < lane for x in col_keys])
    end = count([x <= lane for x in col_keys])
    table[groups : groups + 1, :] = jnp.maximum(end - 1, 0)
    flags[groups : groups + 1, :] = jnp.where(end > begin, 1.0, 0.0)
    for g in range(1, groups):
        cut = jnp.logical_and(begin < g * LANES, end > g * LANES)
        flags[groups + g : groups + g + 1, :] = jnp.where(cut, 1.0, 0.0)

    to_smem = [
        pltpu.make_async_copy(table, order, local_sem.at[1]),
        pltpu.make_async_copy(flags, weight, local_sem.at[5]),
    ]
    for copy in to_smem:
        copy.start()
    for copy in to_smem:
        copy.wait()

    def merge(c):
        rows, top = chunk_rows[c], first_row[c]
        pltpu.make_async_copy(recv[c], recv[c], a2a_recv.at[c]).wait()

        def add(l, running):
            result = []
            for g in range(groups):
                block = recv[c][order[g, l]].astype(jnp.float32)
                total = running[g] * weight[g, l] + block
                partial[g * LANES + l, 0:rows] = total
                result.append(total)
            return tuple(result)

        lax.fori_loop(0, LANES, add, (jnp.zeros((rows, LANES), jnp.float32),) * groups, unroll=UNROLL)
        edges = [partial[g * LANES - 1, 0:rows] for g in range(1, groups)]

        def finish(i, carry):
            a = i // row_blocks
            b = i % row_blocks
            for k in range(col_blocks):
                p = i * col_blocks + k
                total = partial[order[groups, p], 0:rows] * weight[groups, p]
                for g in range(1, groups):
                    total = total + edges[g - 1] * weight[groups + g, p]
                old = base_vmem[a, b, top : top + rows, k * LANES : (k + 1) * LANES]
                stage[c][a, b, :, k * LANES : (k + 1) * LANES] = (old.astype(jnp.float32) + total).astype(jnp.bfloat16)
            return carry

        if c < last:
            lax.fori_loop(0, exp_dev * row_blocks, finish, 0, unroll=FIN_UNROLL)
            return

        def send_segment(i):
            @pl.when(late == 1)
            def _():
                for part in range(SEGMENT_PARTS):
                    first = (i * SEGMENT_PARTS + part) * (exp_dev * row_blocks // SEGMENTS // SEGMENT_PARTS)
                    a, b = divmod(first, row_blocks)
                    blocks = pl.ds(b, exp_dev * row_blocks // SEGMENTS // SEGMENT_PARTS)
                    for shift in [n_dp // 2] + [k for k in range(1, n_dp) if k != n_dp // 2]:
                        pltpu.make_async_remote_copy(
                            src_ref=stage[c].at[a, blocks],
                            dst_ref=out_hbm.at[a, blocks, rows_of(d, c), :],
                            send_sem=gather_send,
                            recv_sem=gather_recv,
                            device_id=(ds[shift], e, m),
                            device_id_type=MESH,
                        ).start()

        size = exp_dev * row_blocks // SEGMENTS
        for i in range(SEGMENTS):
            lax.fori_loop(i * size, (i + 1) * size, finish, 0, unroll=SEG_UNROLL)
            if i > 0:
                send_segment(i - 1)
        send_segment(SEGMENTS - 1)

    for c in range(chunks):
        if c > 0:
            forward(c - 1)
        merge(c)
        gather_own(c)
        if c == last:
            stop = half + AHEAD_LAST
            rest_last = n_steps - stop
            steps(c, stop + rest_last * late, n_steps, gather=c)

            def remaining(t, carry):
                gather_piece(c, t)
                return carry

            lax.fori_loop(rest_last * LAST_STEP + (n_pieces - rest_last * LAST_STEP) * late, n_pieces, remaining, 0)
            continue
        steps(c, early + rest_steps * late, n_steps, gather=c)
        done = rest_steps * core
        stop = early if c + 1 < last else half + AHEAD_LAST
        steps(c + 1, AHEAD * late, stop + (n_steps - stop) * late, gather=c, since=done)
        if c + 2 < chunks:
            done = done + early + (rest_steps - AHEAD) * late
            steps(c + 2, 0, AHEAD * late, gather=c, since=done)

    waited = out_hbm.at[:, :, pl.ds(0, n_dp * quarter - 2 * sum(chunk_rows[:last])), :]
    pltpu.make_async_copy(waited, waited, gather_recv).wait()
    sent = out_hbm.at[:, :, pl.ds(0, (n_dp - 1) * quarter), :]
    pltpu.make_async_copy(sent, sent, gather_send).wait()
    for c in range(chunks):
        sent = recv[c].at[pl.ds(0, n_slots - capacity)]
        pltpu.make_async_copy(sent, sent, a2a_send.at[c]).wait()
    pltpu.make_async_copy(others, others, ids_send.at[0]).wait()
    pltpu.make_async_copy(far_keys, far_keys, ids_send.at[1]).wait()


def body(base_weights, delta_blocks, block_ids, block_counts, owner_map):
    n_dp, n_ex, n_mp = (lax.axis_size(a) for a in ("dp", "expert", "mp"))
    n_dev = n_dp * n_ex * n_mp
    exp_dev, row_count, col_count = base_weights.shape
    block_size = delta_blocks.shape[1]
    row_blocks = row_count // block_size
    col_blocks = col_count // block_size
    capacity = delta_blocks.shape[0] // block_counts.shape[0]
    quarter = block_size // n_dp
    chunk_rows = CHUNKS
    n_slots = n_dev * capacity
    cfg = (n_dp, n_ex, n_mp, exp_dev, row_blocks, col_blocks, capacity, chunk_rows)
    shape = (exp_dev, row_blocks, block_size, col_count)
    filler = jnp.zeros((LANES - block_counts.shape[0] - owner_map.shape[0],), jnp.int32)
    lists = jnp.concatenate([block_ids, block_counts, owner_map, filler]).reshape(2, LANES)
    merged = pl.pallas_call(
        functools.partial(kernel, cfg),
        out_shape=jax.ShapeDtypeStruct(shape, jnp.bfloat16),
        in_specs=[
            pl.BlockSpec(memory_space=pltpu.VMEM),
            pl.BlockSpec(memory_space=pl.ANY),
            pl.BlockSpec(memory_space=pl.ANY),
        ],
        out_specs=pl.BlockSpec(memory_space=pl.ANY),
        scratch_shapes=[
            *[pltpu.VMEM((n_slots, rows, LANES), jnp.bfloat16) for rows in chunk_rows],
            *[pltpu.VMEM((exp_dev, row_blocks, rows, col_count), jnp.bfloat16) for rows in chunk_rows],
            pltpu.VMEM((exp_dev, row_blocks, quarter, col_count), jnp.bfloat16),
            pltpu.VMEM((n_slots, max(chunk_rows), LANES), jnp.float32),
            pltpu.VMEM((1, LANES), jnp.int32),
            pltpu.VMEM((n_ex, 1, LANES), jnp.int32),
            pltpu.VMEM((n_dev, 1, LANES), jnp.int32),
            pltpu.VMEM((LANES, n_dev), jnp.int32),
            pltpu.VMEM((8, LANES), jnp.int32),
            pltpu.VMEM((8, LANES), jnp.float32),
            pltpu.SMEM((8, LANES), jnp.int32),
            pltpu.SMEM((8, LANES), jnp.float32),
            pltpu.SemaphoreType.DMA((len(chunk_rows),)),
            pltpu.SemaphoreType.DMA((len(chunk_rows),)),
            pltpu.SemaphoreType.DMA((2,)),
            pltpu.SemaphoreType.DMA((2,)),
            pltpu.SemaphoreType.DMA((6,)),
            pltpu.SemaphoreType.DMA,
            pltpu.SemaphoreType.DMA,
            pltpu.SemaphoreType.DMA((2 * len(chunk_rows) - 2,)),
            pltpu.SemaphoreType.REGULAR,
        ],
        compiler_params=pltpu.CompilerParams(
            collective_id=0, has_side_effects=True, vmem_limit_bytes=48 * 2**20
        ),
        name="merge_blocks",
    )(
        lists,
        base_weights.reshape(shape),
        delta_blocks,
    )
    return merged.reshape(base_weights.shape)


def solution(mesh):
    in_specs = (
        P("expert", None, "mp"),
        P(("dp", "expert", "mp"), None, None),
        P(("dp", "expert", "mp")),
        P(("dp", "expert", "mp")),
        P(),
    )
    out_specs = P("expert", None, "mp")
    return jax.shard_map(body, mesh=mesh, in_specs=in_specs, out_specs=out_specs, check_vma=False)
```

```python
import functools

import jax
import jax.numpy as jnp
from jax import lax
from jax.experimental import pallas as pl
from jax.experimental.pallas import tpu as pltpu
from jax.sharding import PartitionSpec as P

MESH = pl.DeviceIdType.MESH
CHUNKS = (8, 8, 8, 8)
AHEAD = 16
GATHER_SPLITS = 10
PER_STEP = 4
LAST_STEP = 10
FIN_UNROLL = 8
SEGMENTS = 4
SEGMENT_PARTS = 2
SEG_UNROLL = 10
AHEAD_LAST = 10
UNROLL = 16
LANES = 128


def kernel(
    cfg,
    lists,
    base_hbm,
    delta_hbm,
    out_hbm,
    *scratch,
):
    n_dp, n_ex, n_mp, exp_dev, row_blocks, col_blocks, capacity, chunk_rows = cfg
    chunks = len(chunk_rows)
    first_row = [sum(chunk_rows[:c]) for c in range(chunks)]
    recv = scratch[:chunks]
    stage = scratch[chunks : 2 * chunks]
    (
        base_vmem,
        partial,
        enc,
        column_keys,
        keys,
        keys_t,
        table,
        flags,
        order,
        weight,
        a2a_send,
        a2a_recv,
        ids_send,
        ids_recv,
        local_sem,
        gather_send,
        gather_recv,
        near_recv,
        column_sem,
    ) = scratch[2 * chunks :]
    n_dev = n_dp * n_ex * n_mp
    n_slots = n_dev * capacity
    quarter = sum(chunk_rows)
    positions = exp_dev * row_blocks * col_blocks
    col_total = col_blocks * n_mp
    d = lax.axis_index("dp")
    e = lax.axis_index("expert")
    m = lax.axis_index("mp")
    me = (d * n_mp + m) * n_ex + e

    barrier = pltpu.get_barrier_semaphore()
    ds = [lax.rem(d + i, n_dp) for i in range(n_dp)]
    es = [lax.rem(e + i, n_ex) for i in range(n_ex)]
    ms = [lax.rem(m + i, n_mp) for i in range(n_mp)]
    plane = [(ds[i], e, ms[j]) for j in range(n_mp) for i in range(n_dp) if i or j]
    column = [(d, es[k], m) for k in range(1, n_ex)]
    for device in column + plane:
        pl.semaphore_signal(barrier, inc=1, device_id=device, device_id_type=MESH)

    base_copy = pltpu.make_async_copy(base_hbm.at[:, :, pl.ds(d * quarter, quarter), :], base_vmem, local_sem.at[0])
    base_copy.start()

    ids = lists[0:1, :].astype(jnp.float32)
    counts = lists[1:2, :].astype(jnp.float32)
    owners = n_ex * n_mp
    per_expert = row_blocks * col_total
    expert = jnp.floor((ids + 0.5) * (1.0 / per_expert))
    remain = ids - expert * per_expert
    row_index = jnp.floor((remain + 0.5) * (1.0 / col_total))
    col_index = remain - row_index * col_total
    part = jnp.floor((col_index + 0.5) * (1.0 / col_blocks))
    local_col = col_index - part * col_blocks
    local_expert = jnp.zeros_like(ids)
    for i in range(n_ex * exp_dev):
        position = jnp.broadcast_to(counts[:, owners + i : owners + i + 1], (1, LANES))
        inside = position - exp_dev * jnp.floor(position * (1.0 / exp_dev))
        local_expert = jnp.where(expert == float(i), inside, local_expert)
    place = (local_expert * row_blocks + row_index) * col_blocks + local_col
    spread = (
        lax.broadcasted_iota(jnp.int32, (owners, LANES), 1) // capacity
        == lax.broadcasted_iota(jnp.int32, (owners, LANES), 0)
    ).astype(jnp.float32)
    used = jnp.dot(
        jnp.broadcast_to(counts[:, :owners], (8, owners)), spread, preferred_element_type=jnp.float32
    )[0:1, :]
    slot_k = lax.broadcasted_iota(jnp.int32, (1, LANES), 1) % capacity
    place = jnp.where(slot_k.astype(jnp.float32) < used, place, float(positions))
    enc[...] = place.astype(jnp.int32)

    pl.semaphore_wait(barrier, len(column) + len(plane))
    for device in plane:
        pl.semaphore_signal(column_sem, inc=1, device_id=device, device_id_type=MESH)

    z_order = [n_ex // 2]
    for i in range(n_ex // 2 - 1, 0, -1):
        z_order += [i, n_ex - i]

    def send_block(c, d2, e2, m2):
        q = e2 * n_mp + m2
        pltpu.make_async_remote_copy(
            src_ref=delta_hbm.at[pl.ds(q * capacity, capacity), pl.ds(d2 * quarter + first_row[c], chunk_rows[c]), :],
            dst_ref=recv[c].at[pl.ds(me * capacity, capacity)],
            send_sem=a2a_send.at[c],
            recv_sem=a2a_recv.at[c],
            device_id=(d2, e2, m2),
            device_id_type=MESH,
        ).start()
    mine = e * n_mp + m
    x_count = n_mp // 2
    x = m // 2
    core = m % 2
    late = 1 - core

    n_steps = n_dp * n_mp
    last = chunks - 1
    peers = n_dp - 1
    splits = GATHER_SPLITS
    span = row_blocks // splits
    n_pieces = peers * exp_dev * splits
    half = n_steps // 2
    early = half + AHEAD
    rest_steps = n_steps - early

    def known(c):
        pltpu.make_async_copy(
            delta_hbm.at[pl.ds(mine * capacity, capacity), pl.ds(d * quarter + first_row[c], chunk_rows[c]), :],
            recv[c].at[pl.ds(me * capacity, capacity)],
            a2a_recv.at[c],
        ).start()
        for k in z_order:
            send_block(c, d, es[k], m)
        send_block(c, d, e, m + 1 - 2 * core)

    def steps(c, first, stop, gather=None, since=0):
        def step(r, carry):
            side = 1 - r // half
            rest = lax.rem(r, half)
            d2 = lax.rem(d + rest // x_count, n_dp)
            m2 = lax.rem(x + rest, x_count) * 2 + side

            @pl.when(r != half * late)
            def _():
                for k in z_order:
                    send_block(c, d2, es[k], m2)

            if c == 0:

                @pl.when(rest != 0)
                def _():
                    for other in range(chunks):
                        send_block(other, d2, e, m2)

            gather_pieces(gather, r - first + since, PER_STEP if gather != last else LAST_STEP)
            return carry

        lax.fori_loop(first, stop, step, 0)

    def gather_pieces(c, step, per_step):
        if c is None:
            return
        for k in range(per_step):
            t = step * per_step + k

            @pl.when(t < pieces_of[c])
            def _():
                gather_piece(c, t)

    def rows_of(device, c):
        return pl.ds(device * quarter + first_row[c], chunk_rows[c])

    left, right = ds[n_dp - 1], ds[1]
    pieces_of = [exp_dev * splits * (peers if c == last else 2) for c in range(chunks)]

    def gather_piece(c, t):
        fan = peers if c == last else 2
        piece = t // fan
        a = piece // splits
        part = pl.ds((piece % splits) * span, span)
        to = lax.rem(d + 1 + t % fan * (1 if c == last else n_dp - 2), n_dp)
        arrival = gather_recv if c == last else near_recv.at[c * 2 + t % fan]
        pltpu.make_async_remote_copy(
            src_ref=stage[c].at[a, part],
            dst_ref=out_hbm.at[a, part, rows_of(d, c), :],
            send_sem=gather_send,
            recv_sem=arrival,
            device_id=(to, e, m),
            device_id_type=MESH,
        ).start()

    def forward(c):
        for side in range(2):
            pltpu.make_async_copy(stage[c], stage[c], near_recv.at[c * 2 + side]).wait()

        def step(t, carry):
            part = pl.ds(t * span, span)
            for a in range(exp_dev):
                source, to = (left, right) if a < exp_dev // 2 else (right, left)
                block = out_hbm.at[a, part, rows_of(source, c), :]
                pltpu.make_async_remote_copy(
                    src_ref=block,
                    dst_ref=block,
                    send_sem=gather_send,
                    recv_sem=gather_recv,
                    device_id=(to, e, m),
                    device_id_type=MESH,
                ).start()
            return carry

        lax.fori_loop(0, splits, step, 0)

    def gather_own(c):
        pltpu.make_async_copy(
            stage[c], out_hbm.at[:, :, pl.ds(d * quarter + first_row[c], chunk_rows[c]), :], gather_recv
        ).start()

    for c in range(chunks):
        known(c)
    for k in range(1, n_ex):
        pltpu.make_async_remote_copy(
            src_ref=enc,
            dst_ref=column_keys.at[e],
            send_sem=ids_send.at[0],
            recv_sem=ids_recv.at[0],
            device_id=(d, es[k], m),
            device_id_type=MESH,
        ).start()
    column_keys[pl.ds(e, 1)] = enc[...].reshape(1, 1, LANES)
    pl.semaphore_wait(column_sem, len(plane))
    steps(0, 0, half)
    others = column_keys.at[pl.ds(0, n_ex - 1)]
    pltpu.make_async_copy(others, others, ids_recv.at[0]).wait()
    here = pl.ds((d * n_mp + m) * n_ex, n_ex)
    for device in plane:
        pltpu.make_async_remote_copy(
            src_ref=column_keys,
            dst_ref=keys.at[here],
            send_sem=ids_send.at[1],
            recv_sem=ids_recv.at[1],
            device_id=device,
            device_id_type=MESH,
        ).start()
    keys[here] = column_keys[...]
    steps(0, half, early + rest_steps * late)
    if chunks > 1:
        steps(1, 0, AHEAD * late)
    base_copy.wait()

    far_keys = keys.at[pl.ds(0, n_dev - n_ex)]
    pltpu.make_async_copy(far_keys, far_keys, ids_recv.at[1]).wait()
    all_keys = keys[...].reshape(n_dev, LANES)
    q_mine = e * n_mp + m
    for g in range(n_dev // LANES):
        keys_t[:, g * LANES : (g + 1) * LANES] = all_keys[g * LANES : (g + 1) * LANES, :].T
    lane = lax.broadcasted_iota(jnp.int32, (1, LANES), 1)
    row_keys, row_slots = [], []
    for k in range(capacity):
        row = keys_t[pl.ds(q_mine * capacity + k, 1), :]
        for g in range(n_dev // LANES):
            row_keys.append(row[:, g * LANES : (g + 1) * LANES])
            row_slots.append((g * LANES + lane) * capacity + k)
    groups = len(row_keys)

    def down(row):
        return jnp.broadcast_to(row, (LANES, LANES)).T

    row_mixed = [a * n_slots + b for a, b in zip(row_keys, row_slots)]
    col_keys = [down(a) for a in row_keys]
    col_slots = [down(a) for a in row_slots]
    col_mixed = [a * n_slots + b for a, b in zip(col_keys, col_slots)]

    def count(masks):
        total = sum(jnp.where(x, 1, 0) for x in masks)
        return jnp.sum(total, axis=0, keepdims=True)

    ranks = [count([col_mixed[h] < row_mixed[g] for h in range(groups)]) for g in range(groups)]
    col_ranks = [down(a) for a in ranks]
    for g in range(groups):
        want = g * LANES + lane

        def at(values, rank):
            return jnp.sum(
                sum(jnp.where(r == rank, v, 0) for r, v in zip(col_ranks, values)), axis=0, keepdims=True
            )

        table[g : g + 1, :] = at(col_slots, want)
        same = jnp.logical_and(at(col_keys, want) == at(col_keys, want - 1), lane > 0)
        flags[g : g + 1, :] = jnp.where(same, 1.0, 0.0)
    begin = count([x < lane for x in col_keys])
    end = count([x <= lane for x in col_keys])
    table[groups : groups + 1, :] = jnp.maximum(end - 1, 0)
    flags[groups : groups + 1, :] = jnp.where(end > begin, 1.0, 0.0)
    for g in range(1, groups):
        cut = jnp.logical_and(begin < g * LANES, end > g * LANES)
        flags[groups + g : groups + g + 1, :] = jnp.where(cut, 1.0, 0.0)

    to_smem = [
        pltpu.make_async_copy(table, order, local_sem.at[1]),
        pltpu.make_async_copy(flags, weight, local_sem.at[5]),
    ]
    for copy in to_smem:
        copy.start()
    for copy in to_smem:
        copy.wait()

    def merge(c):
        rows, top = chunk_rows[c], first_row[c]
        pltpu.make_async_copy(recv[c], recv[c], a2a_recv.at[c]).wait()

        def add(l, running):
            result = []
            for g in range(groups):
                block = recv[c][order[g, l]].astype(jnp.float32)
                total = running[g] * weight[g, l] + block
                partial[g * LANES + l, 0:rows] = total
                result.append(total)
            return tuple(result)

        lax.fori_loop(0, LANES, add, (jnp.zeros((rows, LANES), jnp.float32),) * groups, unroll=UNROLL)
        edges = [partial[g * LANES - 1, 0:rows] for g in range(1, groups)]

        def finish(i, carry):
            a = i // row_blocks
            b = i % row_blocks
            for k in range(col_blocks):
                p = i * col_blocks + k
                total = partial[order[groups, p], 0:rows] * weight[groups, p]
                for g in range(1, groups):
                    total = total + edges[g - 1] * weight[groups + g, p]
                old = base_vmem[a, b, top : top + rows, k * LANES : (k + 1) * LANES]
                stage[c][a, b, :, k * LANES : (k + 1) * LANES] = (old.astype(jnp.float32) + total).astype(jnp.bfloat16)
            return carry

        if c < last:
            lax.fori_loop(0, exp_dev * row_blocks, finish, 0, unroll=FIN_UNROLL)
            return

        def send_segment(i):
            @pl.when(late == 1)
            def _():
                for part in range(SEGMENT_PARTS):
                    first = (i * SEGMENT_PARTS + part) * (exp_dev * row_blocks // SEGMENTS // SEGMENT_PARTS)
                    a, b = divmod(first, row_blocks)
                    blocks = pl.ds(b, exp_dev * row_blocks // SEGMENTS // SEGMENT_PARTS)
                    for shift in [n_dp // 2] + [k for k in range(1, n_dp) if k != n_dp // 2]:
                        pltpu.make_async_remote_copy(
                            src_ref=stage[c].at[a, blocks],
                            dst_ref=out_hbm.at[a, blocks, rows_of(d, c), :],
                            send_sem=gather_send,
                            recv_sem=gather_recv,
                            device_id=(ds[shift], e, m),
                            device_id_type=MESH,
                        ).start()

        size = exp_dev * row_blocks // SEGMENTS
        for i in range(SEGMENTS):
            lax.fori_loop(i * size, (i + 1) * size, finish, 0, unroll=SEG_UNROLL)
            if i > 0:
                send_segment(i - 1)
        send_segment(SEGMENTS - 1)

    for c in range(chunks):
        if c > 0:
            forward(c - 1)
        merge(c)
        gather_own(c)
        if c == last:
            stop = half + AHEAD_LAST
            rest_last = n_steps - stop
            steps(c, stop + rest_last * late, n_steps, gather=c)

            def remaining(t, carry):
                gather_piece(c, t)
                return carry

            lax.fori_loop(rest_last * LAST_STEP + (n_pieces - rest_last * LAST_STEP) * late, n_pieces, remaining, 0)
            continue
        steps(c, early + rest_steps * late, n_steps, gather=c)
        done = rest_steps * core
        stop = early if c + 1 < last else half + AHEAD_LAST
        steps(c + 1, AHEAD * late, stop + (n_steps - stop) * late, gather=c, since=done)
        if c + 2 < chunks:
            done = done + early + (rest_steps - AHEAD) * late
            steps(c + 2, 0, AHEAD * late, gather=c, since=done)

    waited = out_hbm.at[:, :, pl.ds(0, n_dp * quarter - 2 * sum(chunk_rows[:last])), :]
    pltpu.make_async_copy(waited, waited, gather_recv).wait()
    sent = out_hbm.at[:, :, pl.ds(0, (n_dp - 1) * quarter), :]
    pltpu.make_async_copy(sent, sent, gather_send).wait()
    for c in range(chunks):
        sent = recv[c].at[pl.ds(0, n_slots - capacity)]
        pltpu.make_async_copy(sent, sent, a2a_send.at[c]).wait()
    pltpu.make_async_copy(others, others, ids_send.at[0]).wait()
    pltpu.make_async_copy(far_keys, far_keys, ids_send.at[1]).wait()


def body(base_weights, delta_blocks, block_ids, block_counts, owner_map):
    n_dp, n_ex, n_mp = (lax.axis_size(a) for a in ("dp", "expert", "mp"))
    n_dev = n_dp * n_ex * n_mp
    exp_dev, row_count, col_count = base_weights.shape
    block_size = delta_blocks.shape[1]
    row_blocks = row_count // block_size
    col_blocks = col_count // block_size
    capacity = delta_blocks.shape[0] // block_counts.shape[0]
    quarter = block_size // n_dp
    chunk_rows = CHUNKS
    n_slots = n_dev * capacity
    cfg = (n_dp, n_ex, n_mp, exp_dev, row_blocks, col_blocks, capacity, chunk_rows)
    shape = (exp_dev, row_blocks, block_size, col_count)
    filler = jnp.zeros((LANES - block_counts.shape[0] - owner_map.shape[0],), jnp.int32)
    lists = jnp.concatenate([block_ids, block_counts, owner_map, filler]).reshape(2, LANES)
    merged = pl.pallas_call(
        functools.partial(kernel, cfg),
        out_shape=jax.ShapeDtypeStruct(shape, jnp.bfloat16),
        in_specs=[
            pl.BlockSpec(memory_space=pltpu.VMEM),
            pl.BlockSpec(memory_space=pl.ANY),
            pl.BlockSpec(memory_space=pl.ANY),
        ],
        out_specs=pl.BlockSpec(memory_space=pl.ANY),
        scratch_shapes=[
            *[pltpu.VMEM((n_slots, rows, LANES), jnp.bfloat16) for rows in chunk_rows],
            *[pltpu.VMEM((exp_dev, row_blocks, rows, col_count), jnp.bfloat16) for rows in chunk_rows],
            pltpu.VMEM((exp_dev, row_blocks, quarter, col_count), jnp.bfloat16),
            pltpu.VMEM((n_slots, max(chunk_rows), LANES), jnp.float32),
            pltpu.VMEM((1, LANES), jnp.int32),
            pltpu.VMEM((n_ex, 1, LANES), jnp.int32),
            pltpu.VMEM((n_dev, 1, LANES), jnp.int32),
            pltpu.VMEM((LANES, n_dev), jnp.int32),
            pltpu.VMEM((8, LANES), jnp.int32),
            pltpu.VMEM((8, LANES), jnp.float32),
            pltpu.SMEM((8, LANES), jnp.int32),
            pltpu.SMEM((8, LANES), jnp.float32),
            pltpu.SemaphoreType.DMA((len(chunk_rows),)),
            pltpu.SemaphoreType.DMA((len(chunk_rows),)),
            pltpu.SemaphoreType.DMA((2,)),
            pltpu.SemaphoreType.DMA((2,)),
            pltpu.SemaphoreType.DMA((6,)),
            pltpu.SemaphoreType.DMA,
            pltpu.SemaphoreType.DMA,
            pltpu.SemaphoreType.DMA((2 * len(chunk_rows) - 2,)),
            pltpu.SemaphoreType.REGULAR,
        ],
        compiler_params=pltpu.CompilerParams(
            collective_id=0, has_side_effects=True, vmem_limit_bytes=48 * 2**20
        ),
        name="merge_blocks",
    )(
        lists,
        base_weights.reshape(shape),
        delta_blocks,
    )
    return merged.reshape(base_weights.shape)


def solution(mesh):
    in_specs = (
        P("expert", None, "mp"),
        P(("dp", "expert", "mp"), None, None),
        P(("dp", "expert", "mp")),
        P(("dp", "expert", "mp")),
        P(),
    )
    out_specs = P("expert", None, "mp")
    return jax.shard_map(body, mesh=mesh, in_specs=in_specs, out_specs=out_specs, check_vma=False)
```
